32 devices in a mesh: rows: 8 (over z, y), dp: 4 (over x, core).
Axes of the slice: x: 2, y: 2, z: 4, core: 2. Of those that a mesh axis runs over, the one named last changes fastest.
Arguments:
- weights: float32 [6144, 4096], P(('rows', 'dp'))
- moment: float32 [6144, 4096], P(('rows', 'dp'))
- second: float32 [6144, 4096], P(('rows', 'dp')), may hold values from 0.01 to 1
- tile_rows: bfloat16 [2048, 4096], P(('rows', 'dp')), may hold values from -6 to 6
- row_index: int32 [2048], P(('rows', 'dp')), may hold values from 0 to 191
- bucket_count: int32 [1024], P(('rows', 'dp')), may hold values from 1 to 2, as said below
Outputs:
- new_weights: float32 [6144, 4096], P(('rows', 'dp'))
- new_moment: float32 [6144, 4096], P(('rows', 'dp'))
- new_second: float32 [6144, 4096], P(('rows', 'dp'))
The draws below stay inside these ranges and needn't reach their ends.
Inputs may be any that keep to these rules, and one draw needn't show every extreme that they name: `bucket_count`: at least one slot of every sender and owner is live; in every draw some owner receives 2 live slots from every sender. `row_index`: rows may repeat within and across senders.
All inputs are finite; a program needn't handle non-finite values.
Results may differ from the reference program's by a relative error of at most 0.0003.
Values may be sent and summed in bfloat16 or wider, within the bound.
No kernel may reach another device: no remote copies, remote signals or barrier semaphores. Data moves between devices by JAX's collectives and lax.ppermute only.
A program may use at most 64 MiB of HBM per device.

```python
import math
import jax
import jax.numpy as jnp

D = 4096
ROWS_DEV = 192
CAP = 2
OWNERS = 32
VOCAB = 6144
SLOTS = 64


def draw_weights(key, part):
    key_one = jax.random.fold_in(key, 21)
    key_two = jax.random.fold_in(key, 22)
    key_three = jax.random.fold_in(key, 23)
    row_pos = jnp.arange(VOCAB, dtype=jnp.float32) / VOCAB
    normal_part = jax.random.truncated_normal(key_one, -4.0, 4.0, (VOCAB, D), jnp.float32)
    row_scale = 10.0 ** jax.random.uniform(key_two, (VOCAB, 1), jnp.float32) * 3.0 ** row_pos[:, None]
    col_scale = 10.0 ** jax.random.uniform(key_three, (1, D), jnp.float32)
    return 0.05 * normal_part * row_scale * col_scale


def draw_moment(key, part):
    key_one = jax.random.fold_in(key, 31)
    key_two = jax.random.fold_in(key, 32)
    row_pos = jnp.arange(VOCAB, dtype=jnp.float32) / VOCAB
    normal_part = jax.random.truncated_normal(key_one, -4.0, 4.0, (VOCAB, D), jnp.float32)
    row_scale = 10.0 ** jax.random.uniform(key_two, (VOCAB, 1), jnp.float32) * 3.0 ** row_pos[:, None]
    return 0.05 * normal_part * row_scale


def draw_bucket_count(key, part):
    key_one = jax.random.fold_in(key, 11)
    key_two = jax.random.fold_in(key, 12)
    counts_all = jax.random.randint(key_one, (OWNERS, OWNERS), 1, CAP + 1)
    full_owner = jax.random.randint(key_two, (), 0, OWNERS)
    column_id = jnp.arange(OWNERS)[None, :]
    return jnp.where(column_id == full_owner, CAP, counts_all).reshape(-1).astype(jnp.int32)


def touch_ends(entries, stream_key, least, largest):
    spot = [jax.random.randint(jax.random.fold_in(stream_key, axis), (), 0, length) for axis, length in enumerate(entries.shape)]
    widest = entries.shape.index(max(entries.shape))
    next_to = spot[:widest] + [(spot[widest] + 1) % entries.shape[widest]] + spot[widest + 1:]
    return entries.at[tuple(spot)].set(least).at[tuple(next_to)].set(largest)


def steps_of(stream_key, extent, split, least, largest):
    factor_of = 1.0
    for dim, shards_of in split:
        steps = jax.random.uniform(jax.random.fold_in(jax.random.fold_in(stream_key, 6), dim), (shards_of,), jnp.float32, least / len(split), largest / len(split))
        factor_of = factor_of * jnp.repeat(jnp.exp(steps), extent[dim] // shards_of).reshape((-1,) + (1,) * (len(extent) - 1 - dim))
    return factor_of


def gaussian(stream_key, extent, scale, limit, shards=(), kind=jnp.bfloat16):
    loudness = steps_of(stream_key, extent, shards, -0.22, 0.18) if shards else 1.0
    array = jax.random.normal(stream_key, extent, jnp.float32) * scale * loudness
    return jnp.minimum(jnp.maximum(array, -limit), limit).astype(kind)


def setup_inputs(seed: int = 0) -> dict:
    streams_of = jax.random.split(jax.random.key(seed), 7)
    return {
        "weights": draw_weights(jax.random.fold_in(streams_of[6], 71), 0),
        "moment": draw_moment(jax.random.fold_in(streams_of[6], 71), 0),
        "second": jnp.clip(jnp.exp(math.log(1.0) - 4.6051702 * jax.random.uniform(streams_of[2], (VOCAB, D), jnp.float32) ** steps_of(streams_of[2], (VOCAB, D), ((0, 32),), -0.2, 0.2)), 0.01, 1.0),
        "tile_rows": gaussian(streams_of[3], (OWNERS * SLOTS, D), 1.0, 6.0, ((0, 32),)),
        "row_index": touch_ends(jax.random.randint(streams_of[4], (OWNERS * SLOTS,), 0, ROWS_DEV), jax.random.fold_in(streams_of[4], 1), 0, ROWS_DEV - 1).astype(jnp.int32),
        "bucket_count": draw_bucket_count(jax.random.fold_in(streams_of[6], 71), 0),
    }


beta_one = 0.9
beta_two = 0.999
epsilon = 1e-06
decay = 0.01
rate = 0.1

def reference(weights, moment, second, tile_rows, row_index, bucket_count):
    position = jnp.arange(OWNERS * SLOTS, dtype=jnp.int32)
    slot_pos = position % CAP
    bucket_id = position // CAP
    owner_id = bucket_id % OWNERS
    is_live = slot_pos < bucket_count[bucket_id]
    table_row = jnp.where(is_live, owner_id * ROWS_DEV + row_index, 0).astype(jnp.int32)
    values = tile_rows.astype(jnp.float32) * is_live.astype(jnp.float32)[:, None]
    gradient = jax.ops.segment_sum(values, table_row, num_segments=VOCAB)
    new_moment = beta_one * moment + (1.0 - beta_one) * gradient
    new_second = beta_two * second + (1.0 - beta_two) * gradient * gradient
    update = new_moment / (jnp.sqrt(new_second) + epsilon) + decay * weights
    weight_sq = jnp.sum(weights * weights)
    update_sq = jnp.sum(update * update)
    trust_ratio = jnp.sqrt(weight_sq) / jnp.sqrt(update_sq + 1e-06)
    new_weights = weights - rate * trust_ratio * update
    return (new_weights, new_moment, new_second)
```

```python
import jax
import jax.numpy as jnp
from jax import lax
from jax.sharding import PartitionSpec as P

beta_one = 0.9
beta_two = 0.999
epsilon = 1e-06
decay = 0.01
rate = 0.1
LANES = 128
AXES = ("rows", "dp")


def local(weights, moment, second, tile_rows, row_index, bucket_count):
    owners = lax.axis_size(AXES)
    rows_here, width = weights.shape
    slot_total = row_index.shape[0]
    capacity = slot_total // owners
    is_live = lax.broadcasted_iota(jnp.int32, (owners, capacity), 1) < bucket_count[:, None]
    target = jnp.where(is_live, row_index.reshape(owners, capacity), -1)[:, :, None]
    lane = lax.broadcasted_iota(jnp.int32, (owners, capacity, LANES), 2)
    digits = jnp.where(lane == 0, target >> 7, target & 127).astype(jnp.bfloat16)
    packed = jnp.concatenate([tile_rows.reshape(owners, capacity, width), digits], axis=2)
    arrived = lax.all_to_all(packed, AXES, split_axis=0, concat_axis=0, tiled=True)
    arrived = arrived.reshape(slot_total, width + LANES)
    landing = arrived[:, width].astype(jnp.int32) * 128 + arrived[:, width + 1].astype(jnp.int32)
    picker = (
        landing[None, :] == lax.broadcasted_iota(jnp.int32, (rows_here, slot_total), 0)
    ).astype(jnp.bfloat16)
    gradient = jnp.dot(picker, arrived[:, :width], preferred_element_type=jnp.float32)
    new_moment = beta_one * moment + (1.0 - beta_one) * gradient
    new_second = beta_two * second + (1.0 - beta_two) * gradient * gradient
    update = new_moment / (jnp.sqrt(new_second) + epsilon) + decay * weights
    parts = jnp.stack([jnp.sum(weights * weights), jnp.sum(update * update)])
    told = jnp.broadcast_to(parts[None, :, None], (owners, 2, LANES))
    heard = lax.all_to_all(told, AXES, split_axis=0, concat_axis=0, tiled=True)
    sums = jnp.sum(heard[:, :, 0], axis=0)
    trust_ratio = jnp.sqrt(sums[0]) / jnp.sqrt(sums[1] + 1e-06)
    new_weights = weights - rate * trust_ratio * update
    return (new_weights, new_moment, new_second)


def solution(mesh):
    placed = (P(AXES, None),) * 4 + (P(AXES),) * 2
    return jax.shard_map(
        local, mesh=mesh, in_specs=placed, out_specs=(P(AXES, None),) * 3, check_vma=False
    )
```

```python
import functools
import math

import jax
import jax.numpy as jnp
from jax import lax
from jax.experimental import pallas as pl
from jax.experimental.pallas import tpu as pltpu
from jax.sharding import PartitionSpec as P

beta_one = 0.9
beta_two = 0.999
epsilon = 1e-06
decay = 0.01
rate = 0.1
LANES = 128
AXES = ("rows", "dp")
MIB = 1 << 20

VMEM = pl.BlockSpec(memory_space=pltpu.VMEM)
SMEM = pl.BlockSpec(memory_space=pltpu.SMEM)
ANY = pl.BlockSpec(memory_space=pl.ANY)


def cost(flops):
    return pl.CostEstimate(flops=flops, bytes_accessed=0, transcendentals=0)


def start(token_ref):
    token_ref[...] = jnp.zeros_like(token_ref)


def address(token_ref, index_ref, count_ref, out_ref):
    del token_ref
    owners, capacity, lanes = out_ref.shape
    slots = owners * capacity
    slot = lax.broadcasted_iota(jnp.int32, (slots, slots), 0)
    across = lax.broadcasted_iota(jnp.int32, (slots, slots), 1)
    index = jnp.broadcast_to(index_ref[...].reshape(1, slots), (slots, slots))
    index = jnp.sum(jnp.where(slot == across, index, 0), axis=1, keepdims=True)
    owner = lax.broadcasted_iota(jnp.int32, (slots, owners), 0) // capacity
    across = lax.broadcasted_iota(jnp.int32, (slots, owners), 1)
    count = jnp.broadcast_to(count_ref[...].reshape(1, owners), (slots, owners))
    count = jnp.sum(jnp.where(owner == across, count, 0), axis=1, keepdims=True)
    place = lax.broadcasted_iota(jnp.int32, (slots, 1), 0) % capacity
    target = jnp.broadcast_to(jnp.where(place < count, index, -1), (slots, lanes))
    lane = lax.broadcasted_iota(jnp.int32, (slots, lanes), 1)
    digits = jnp.where(lane == 0, target >> 7, target & 127)
    digits = digits.astype(jnp.float32).astype(jnp.bfloat16)
    out_ref[...] = digits.reshape(owners, capacity, lanes)


def pack(digits_ref, tile_ref, out_ref):
    owners, capacity, padded = out_ref.shape
    width = padded - LANES
    out_ref[:, :, width:] = digits_ref[...]
    out_ref[:, :, :width] = tile_ref[...].reshape(owners, capacity, width)


def advance(block, tile, arrived_ref, weights_ref, moment_ref, second_ref,
            new_moment_hbm, new_second_hbm, update_ref, told_ref,
            new_moment_ref, new_second_ref, even_ref, odd_ref, sem):
    rows_here, width = weights_ref.shape
    owners, capacity, _ = arrived_ref.shape
    slots = owners * capacity
    blocks = width // block
    digits = arrived_ref[:, :, width:].reshape(slots, LANES).astype(jnp.float32)
    landing = (digits[:, 0:1] * 128.0 + digits[:, 1:2]).astype(jnp.int32)
    picker = (
        landing == lax.broadcasted_iota(jnp.int32, (slots, rows_here), 1)
    ).astype(jnp.float32).T.astype(jnp.bfloat16)

    def gather(j, gradient_ref):
        for k in range(0, block, tile):
            sent = arrived_ref[:, :, j * block + k:j * block + k + tile].reshape(slots, tile)
            gradient_ref[:, k:k + tile] = jnp.dot(picker, sent, preferred_element_type=jnp.float32)

    weight_sum = jnp.zeros((8, block), jnp.float32)
    update_sum = jnp.zeros((8, block), jnp.float32)
    stores = []
    gather(0, even_ref)
    for j in range(blocks):
        gradient_ref, next_ref = (even_ref, odd_ref) if j % 2 == 0 else (odd_ref, even_ref)
        if j + 1 < blocks:
            gather(j + 1, next_ref)
        cols = pl.ds(j * block, block)
        for r in range(0, rows_here, 8):
            rows = pl.ds(r, 8)
            gradient = gradient_ref[rows, :]
            weights = weights_ref[rows, cols]
            new_moment = beta_one * moment_ref[rows, cols] + (1.0 - beta_one) * gradient
            new_second = beta_two * second_ref[rows, cols] + (1.0 - beta_two) * gradient * gradient
            root = new_second * lax.rsqrt(new_second)
            update = new_moment / (root + epsilon) + decay * weights
            new_moment_ref[rows, cols] = new_moment
            new_second_ref[rows, cols] = new_second
            update_ref[rows, cols] = update
            weight_sum += weights * weights
            update_sum += update * update
        for k, (held, out) in enumerate(((new_moment_ref, new_moment_hbm), (new_second_ref, new_second_hbm))):
            stores.append(pltpu.make_async_copy(held.at[:, cols], out.at[:, cols], sem.at[k, j]))
            stores[-1].start()

    def narrow(x):
        x = jnp.sum(x, axis=0, keepdims=True)
        return sum(x[:, k:k + LANES] for k in range(0, block, LANES))

    both = jnp.concatenate([narrow(weight_sum), narrow(update_sum)], axis=0)
    told_ref[...] = jnp.broadcast_to(both[None], told_ref.shape)
    for store in stores:
        store.wait()


def apply(chunk, heard_ref, weights_ref, update_ref, out_ref, held_ref, sem):
    sums = jnp.sum(jnp.sum(heard_ref[...], axis=0), axis=1, keepdims=True)
    scale = rate * (jnp.sqrt(sums[0:1]) / jnp.sqrt(sums[1:2] + 1e-06))
    stores = []
    for k in range(weights_ref.shape[0] // chunk):
        rows = pl.ds(k * chunk, chunk)
        held_ref[rows, :] = weights_ref[rows, :] - scale * update_ref[rows, :]
        stores.append(pltpu.make_async_copy(held_ref.at[rows, :], out_ref.at[rows, :], sem.at[k]))
        stores[-1].start()
    for store in stores:
        store.wait()


def local(weights, moment, second, tile_rows, row_index, bucket_count):
    owners = lax.axis_size(AXES)
    rows_here, width = weights.shape
    slot_total = row_index.shape[0]
    capacity = slot_total // owners
    block = math.gcd(width, 512)
    tile = math.gcd(width, 256)
    chunk = 24
    table = jax.ShapeDtypeStruct((rows_here, width), jnp.float32)
    token = pl.pallas_call(
        start,
        out_shape=jax.ShapeDtypeStruct((8, LANES), jnp.float32),
        out_specs=VMEM,
        compiler_params=pltpu.CompilerParams(vmem_limit_bytes=MIB),
        cost_estimate=cost(10000000000),
        name="start",
    )()
    digits = pl.pallas_call(
        address,
        out_shape=jax.ShapeDtypeStruct((owners, capacity, LANES), jnp.bfloat16),
        in_specs=[VMEM] * 3,
        out_specs=VMEM,
        compiler_params=pltpu.CompilerParams(vmem_limit_bytes=4 * MIB),
        cost_estimate=cost(1000000),
        name="address",
    )(token, row_index, bucket_count)
    packed = pl.pallas_call(
        pack,
        out_shape=jax.ShapeDtypeStruct((owners, capacity, width + LANES), jnp.bfloat16),
        in_specs=[VMEM] * 2,
        out_specs=VMEM,
        compiler_params=pltpu.CompilerParams(vmem_limit_bytes=16 * MIB),
        cost_estimate=cost(10000000000),
        name="pack",
    )(digits, tile_rows)
    arrived = lax.all_to_all(packed, AXES, split_axis=0, concat_axis=0, tiled=True)
    new_moment, new_second, update, told = pl.pallas_call(
        functools.partial(advance, block, tile),
        out_shape=(table,) * 3 + (jax.ShapeDtypeStruct((owners, 2, LANES), jnp.float32),),
        in_specs=[VMEM] * 4,
        out_specs=(ANY, ANY, VMEM, VMEM),
        scratch_shapes=[
            pltpu.VMEM((rows_here, width), jnp.float32),
            pltpu.VMEM((rows_here, width), jnp.float32),
            pltpu.VMEM((rows_here, block), jnp.float32),
            pltpu.VMEM((rows_here, block), jnp.float32),
            pltpu.SemaphoreType.DMA((2, width // block)),
        ],
        compiler_params=pltpu.CompilerParams(vmem_limit_bytes=32 * MIB),
        cost_estimate=cost(100000000),
        name="advance",
    )(arrived, weights, moment, second)
    heard = lax.all_to_all(told, AXES, split_axis=0, concat_axis=0, tiled=True)
    new_weights = pl.pallas_call(
        functools.partial(apply, chunk),
        out_shape=table,
        in_specs=[VMEM] * 3,
        out_specs=ANY,
        scratch_shapes=[
            pltpu.VMEM((rows_here, width), jnp.float32),
            pltpu.SemaphoreType.DMA((rows_here // chunk,)),
        ],
        compiler_params=pltpu.CompilerParams(vmem_limit_bytes=24 * MIB),
        cost_estimate=cost(1000000),
        name="apply",
    )(heard, weights, update)
    return (new_weights, new_moment, new_second)


def solution(mesh):
    placed = (P(AXES, None),) * 4 + (P(AXES),) * 2
    return jax.shard_map(
        local, mesh=mesh, in_specs=placed, out_specs=(P(AXES, None),) * 3, check_vma=False
    )
```

```python
import functools
import math

import jax
import jax.numpy as jnp
from jax import lax
from jax.experimental import pallas as pl
from jax.experimental.pallas import tpu as pltpu
from jax.sharding import PartitionSpec as P

beta_one = 0.9
beta_two = 0.999
epsilon = 1e-06
decay = 0.01
rate = 0.1
LANES = 128
AXES = ("rows", "dp")
MIB = 1 << 20

VMEM = pl.BlockSpec(memory_space=pltpu.VMEM)
SMEM = pl.BlockSpec(memory_space=pltpu.SMEM)
ANY = pl.BlockSpec(memory_space=pl.ANY)


def cost(flops):
    return pl.CostEstimate(flops=flops, bytes_accessed=0, transcendentals=0)


def start(token_ref):
    token_ref[...] = jnp.zeros_like(token_ref)


def address(token_ref, index_ref, count_ref, out_ref):
    del token_ref
    owners, capacity, lanes = out_ref.shape
    slots = owners * capacity
    slot = lax.broadcasted_iota(jnp.int32, (slots, slots), 0)
    across = lax.broadcasted_iota(jnp.int32, (slots, slots), 1)
    index = jnp.broadcast_to(index_ref[...].reshape(1, slots), (slots, slots))
    index = jnp.sum(jnp.where(slot == across, index, 0), axis=1, keepdims=True)
    owner = lax.broadcasted_iota(jnp.int32, (slots, owners), 0) // capacity
    across = lax.broadcasted_iota(jnp.int32, (slots, owners), 1)
    count = jnp.broadcast_to(count_ref[...].reshape(1, owners), (slots, owners))
    count = jnp.sum(jnp.where(owner == across, count, 0), axis=1, keepdims=True)
    place = lax.broadcasted_iota(jnp.int32, (slots, 1), 0) % capacity
    target = jnp.broadcast_to(jnp.where(place < count, index, -1), (slots, lanes))
    lane = lax.broadcasted_iota(jnp.int32, (slots, lanes), 1)
    digits = jnp.where(lane == 0, target >> 7, target & 127)
    digits = digits.astype(jnp.float32).astype(jnp.bfloat16)
    out_ref[...] = digits.reshape(owners, capacity, lanes)


def pack(digits_ref, tile_ref, out_ref):
    owners, capacity, padded = out_ref.shape
    width = padded - LANES
    out_ref[:, :, width:] = digits_ref[...]
    out_ref[:, :, :width] = tile_ref[...].reshape(owners, capacity, width)


def advance(block, tile, arrived_ref, weights_ref, moment_ref, second_ref,
            new_moment_hbm, new_second_hbm, late_moment_ref, late_second_ref, update_ref, told_ref,
            new_moment_ref, new_second_ref, even_ref, odd_ref, sem):
    rows_here, width = weights_ref.shape
    owners, capacity, _ = arrived_ref.shape
    slots = owners * capacity
    blocks = width // block
    digits = arrived_ref[:, :, width:].reshape(slots, LANES).astype(jnp.float32)
    landing = (digits[:, 0:1] * 128.0 + digits[:, 1:2]).astype(jnp.int32)
    picker = (
        landing == lax.broadcasted_iota(jnp.int32, (slots, rows_here), 1)
    ).astype(jnp.float32).T.astype(jnp.bfloat16)

    def gather(j, gradient_ref):
        for k in range(0, block, tile):
            sent = arrived_ref[:, :, j * block + k:j * block + k + tile].reshape(slots, tile)
            gradient_ref[:, k:k + tile] = jnp.dot(picker, sent, preferred_element_type=jnp.float32)

    weight_sum = jnp.zeros((8, block), jnp.float32)
    update_sum = jnp.zeros((8, block), jnp.float32)
    stores = []
    gather(0, even_ref)
    for j in range(blocks):
        gradient_ref, next_ref = (even_ref, odd_ref) if j % 2 == 0 else (odd_ref, even_ref)
        if j + 1 < blocks:
            gather(j + 1, next_ref)
        cols = pl.ds(j * block, block)
        late = j + 1 == blocks
        moment_to, second_to = (late_moment_ref, late_second_ref) if late else (new_moment_ref, new_second_ref)
        into = pl.ds(0, block) if late else cols
        for r in range(0, rows_here, 8):
            rows = pl.ds(r, 8)
            gradient = gradient_ref[rows, :]
            weights = weights_ref[rows, cols]
            new_moment = beta_one * moment_ref[rows, cols] + (1.0 - beta_one) * gradient
            new_second = beta_two * second_ref[rows, cols] + (1.0 - beta_two) * gradient * gradient
            root = new_second * lax.rsqrt(new_second)
            update = new_moment / (root + epsilon) + decay * weights
            moment_to[rows, into] = new_moment
            second_to[rows, into] = new_second
            update_ref[rows, cols] = update
            weight_sum += weights * weights
            update_sum += update * update
        if late:
            continue
        for k, (held, out) in enumerate(((new_moment_ref, new_moment_hbm), (new_second_ref, new_second_hbm))):
            stores.append(pltpu.make_async_copy(held.at[:, cols], out.at[:, cols], sem.at[k, j]))
            stores[-1].start()

    def narrow(x):
        x = jnp.sum(x, axis=0, keepdims=True)
        return sum(x[:, k:k + LANES] for k in range(0, block, LANES))

    both = jnp.concatenate([narrow(weight_sum), narrow(update_sum)], axis=0)
    told_ref[...] = jnp.broadcast_to(both[None], told_ref.shape)
    for store in stores:
        store.wait()


def apply(chunk, heard_ref, weights_ref, update_ref, late_moment_ref, late_second_ref, moment_in, second_in,
          out_ref, new_moment_hbm, new_second_hbm, held_ref, sem):
    del moment_in, second_in
    rows_here, width = weights_ref.shape
    block = late_moment_ref.shape[1]
    cols = pl.ds(width - block, block)
    stores = [
        pltpu.make_async_copy(late_moment_ref, new_moment_hbm.at[:, cols], sem.at[0]),
        pltpu.make_async_copy(late_second_ref, new_second_hbm.at[:, cols], sem.at[1]),
    ]
    for store in stores:
        store.start()
    sums = jnp.sum(jnp.sum(heard_ref[...], axis=0), axis=1, keepdims=True)
    scale = rate * (jnp.sqrt(sums[0:1]) / jnp.sqrt(sums[1:2] + 1e-06))
    for k in range(rows_here // chunk):
        rows = pl.ds(k * chunk, chunk)
        held_ref[rows, :] = weights_ref[rows, :] - scale * update_ref[rows, :]
        stores.append(pltpu.make_async_copy(held_ref.at[rows, :], out_ref.at[rows, :], sem.at[2 + k]))
        stores[-1].start()
    for store in stores:
        store.wait()


def local(weights, moment, second, tile_rows, row_index, bucket_count):
    owners = lax.axis_size(AXES)
    rows_here, width = weights.shape
    slot_total = row_index.shape[0]
    capacity = slot_total // owners
    block = math.gcd(width, 512)
    tile = math.gcd(width, 256)
    chunk = 24
    table = jax.ShapeDtypeStruct((rows_here, width), jnp.float32)
    token = pl.pallas_call(
        start,
        out_shape=jax.ShapeDtypeStruct((8, LANES), jnp.float32),
        out_specs=VMEM,
        compiler_params=pltpu.CompilerParams(vmem_limit_bytes=MIB),
        cost_estimate=cost(10000000000),
        name="start",
    )()
    digits = pl.pallas_call(
        address,
        out_shape=jax.ShapeDtypeStruct((owners, capacity, LANES), jnp.bfloat16),
        in_specs=[VMEM] * 3,
        out_specs=VMEM,
        compiler_params=pltpu.CompilerParams(vmem_limit_bytes=4 * MIB),
        cost_estimate=cost(1000000),
        name="address",
    )(token, row_index, bucket_count)
    packed = pl.pallas_call(
        pack,
        out_shape=jax.ShapeDtypeStruct((owners, capacity, width + LANES), jnp.bfloat16),
        in_specs=[VMEM] * 2,
        out_specs=VMEM,
        compiler_params=pltpu.CompilerParams(vmem_limit_bytes=16 * MIB),
        cost_estimate=cost(10000000000),
        name="pack",
    )(digits, tile_rows)
    arrived = lax.all_to_all(packed, AXES, split_axis=0, concat_axis=0, tiled=True)
    late = jax.ShapeDtypeStruct((rows_here, block), jnp.float32)
    new_moment, new_second, late_moment, late_second, update, told = pl.pallas_call(
        functools.partial(advance, block, tile),
        out_shape=(table, table, late, late, table, jax.ShapeDtypeStruct((owners, 2, LANES), jnp.float32)),
        in_specs=[VMEM] * 4,
        out_specs=(ANY, ANY) + (VMEM,) * 4,
        scratch_shapes=[
            pltpu.VMEM((rows_here, width), jnp.float32),
            pltpu.VMEM((rows_here, width), jnp.float32),
            pltpu.VMEM((rows_here, block), jnp.float32),
            pltpu.VMEM((rows_here, block), jnp.float32),
            pltpu.SemaphoreType.DMA((2, width // block)),
        ],
        compiler_params=pltpu.CompilerParams(vmem_limit_bytes=32 * MIB),
        cost_estimate=cost(100000000),
        name="advance",
    )(arrived, weights, moment, second)
    heard = lax.all_to_all(told, AXES, split_axis=0, concat_axis=0, tiled=True)
    return pl.pallas_call(
        functools.partial(apply, chunk),
        out_shape=(table,) * 3,
        in_specs=[VMEM] * 5 + [ANY] * 2,
        out_specs=(ANY,) * 3,
        input_output_aliases={5: 1, 6: 2},
        scratch_shapes=[
            pltpu.VMEM((rows_here, width), jnp.float32),
            pltpu.SemaphoreType.DMA((2 + rows_here // chunk,)),
        ],
        compiler_params=pltpu.CompilerParams(vmem_limit_bytes=24 * MIB),
        cost_estimate=cost(1000000),
        name="apply",
    )(heard, weights, update, late_moment, late_second, new_moment, new_second)


def solution(mesh):
    placed = (P(AXES, None),) * 4 + (P(AXES),) * 2
    return jax.shard_map(
        local, mesh=mesh, in_specs=placed, out_specs=(P(AXES, None),) * 3, check_vma=False
    )
```

```python
import functools
import math

import jax
import jax.numpy as jnp
from jax import lax
from jax.experimental import pallas as pl
from jax.experimental.pallas import tpu as pltpu
from jax.sharding import PartitionSpec as P

beta_one = 0.9
beta_two = 0.999
epsilon = 1e-06
decay = 0.01
rate = 0.1
LANES = 128
AXES = ("rows", "dp")
MIB = 1 << 20

VMEM = pl.BlockSpec(memory_space=pltpu.VMEM)
ANY = pl.BlockSpec(memory_space=pl.ANY)


def cost(flops):
    return pl.CostEstimate(flops=flops, bytes_accessed=0, transcendentals=0)


def start(token_ref):
    token_ref[...] = jnp.zeros_like(token_ref)


def address(token_ref, index_ref, count_ref, out_ref):
    del token_ref
    owners, capacity, lanes = out_ref.shape
    slots = owners * capacity
    slot = lax.broadcasted_iota(jnp.int32, (slots, slots), 0)
    across = lax.broadcasted_iota(jnp.int32, (slots, slots), 1)
    index = jnp.broadcast_to(index_ref[...].reshape(1, slots), (slots, slots))
    index = jnp.sum(jnp.where(slot == across, index, 0), axis=1, keepdims=True)
    owner = lax.broadcasted_iota(jnp.int32, (slots, owners), 0) // capacity
    across = lax.broadcasted_iota(jnp.int32, (slots, owners), 1)
    count = jnp.broadcast_to(count_ref[...].reshape(1, owners), (slots, owners))
    count = jnp.sum(jnp.where(owner == across, count, 0), axis=1, keepdims=True)
    place = lax.broadcasted_iota(jnp.int32, (slots, 1), 0) % capacity
    target = jnp.broadcast_to(jnp.where(place < count, index, -1), (slots, lanes))
    lane = lax.broadcasted_iota(jnp.int32, (slots, lanes), 1)
    digits = jnp.where(lane == 0, target >> 7, target & 127)
    digits = digits.astype(jnp.float32).astype(jnp.bfloat16)
    out_ref[...] = digits.reshape(owners, capacity, lanes)


def pack(digits_ref, tile_ref, out_ref):
    owners, capacity, padded = out_ref.shape
    width = padded - LANES
    out_ref[:, :, width:] = digits_ref[...]
    out_ref[:, :, :width] = tile_ref[...].reshape(owners, capacity, width)


def advance(block, tile, arrived_ref, weights_ref, moment_ref, second_ref,
            new_moment_hbm, new_second_hbm, late_moment_ref, late_second_ref, update_ref, told_ref,
            new_moment_ref, new_second_ref, even_ref, odd_ref, sem):
    rows_here, width = weights_ref.shape
    owners, capacity, _ = arrived_ref.shape
    slots = owners * capacity
    blocks = width // block
    digits = arrived_ref[:, :, width:].reshape(slots, LANES).astype(jnp.float32)
    landing = (digits[:, 0:1] * 128.0 + digits[:, 1:2]).astype(jnp.int32)
    picker = (
        landing == lax.broadcasted_iota(jnp.int32, (slots, rows_here), 1)
    ).astype(jnp.float32).T.astype(jnp.bfloat16)

    def gather(j, gradient_ref):
        for k in range(0, block, tile):
            sent = arrived_ref[:, :, j * block + k:j * block + k + tile].reshape(slots, tile)
            gradient_ref[:, k:k + tile] = jnp.dot(picker, sent, preferred_element_type=jnp.float32)

    weight_sum = jnp.zeros((8, block), jnp.float32)
    update_sum = jnp.zeros((8, block), jnp.float32)
    stores = []
    gather(0, even_ref)
    for j in range(blocks):
        gradient_ref, next_ref = (even_ref, odd_ref) if j % 2 == 0 else (odd_ref, even_ref)
        if j + 1 < blocks:
            gather(j + 1, next_ref)
        cols = pl.ds(j * block, block)
        late = j + 1 == blocks
        moment_to, second_to = (late_moment_ref, late_second_ref) if late else (new_moment_ref, new_second_ref)
        into = pl.ds(0, block) if late else cols
        for r in range(0, rows_here, 8):
            rows = pl.ds(r, 8)
            gradient = gradient_ref[rows, :]
            weights = weights_ref[rows, cols]
            new_moment = beta_one * moment_ref[rows, cols] + (1.0 - beta_one) * gradient
            new_second = beta_two * second_ref[rows, cols] + (1.0 - beta_two) * gradient * gradient
            root = new_second * lax.rsqrt(new_second)
            update = new_moment / (root + epsilon) + decay * weights
            moment_to[rows, into] = new_moment
            second_to[rows, into] = new_second
            update_ref[rows, cols] = update
            weight_sum += weights * weights
            update_sum += update * update
        if late:
            continue
        for k, (held, out) in enumerate(((new_moment_ref, new_moment_hbm), (new_second_ref, new_second_hbm))):
            stores.append(pltpu.make_async_copy(held.at[:, cols], out.at[:, cols], sem.at[k, j]))
            stores[-1].start()

    def narrow(x):
        x = jnp.sum(x, axis=0, keepdims=True)
        return sum(x[:, k:k + LANES] for k in range(0, block, LANES))

    both = jnp.concatenate([narrow(weight_sum), narrow(update_sum)], axis=0)
    told_ref[...] = jnp.broadcast_to(both[None], told_ref.shape)
    for store in stores:
        store.wait()


def apply(chunk, heard_ref, weights_ref, update_ref, late_moment_ref, late_second_ref, moment_in, second_in,
          out_ref, new_moment_hbm, new_second_hbm, held_ref, sem):
    del moment_in, second_in
    rows_here, width = weights_ref.shape
    block = late_moment_ref.shape[1]
    cols = pl.ds(width - block, block)
    stores = [
        pltpu.make_async_copy(late_moment_ref, new_moment_hbm.at[:, cols], sem.at[0]),
        pltpu.make_async_copy(late_second_ref, new_second_hbm.at[:, cols], sem.at[1]),
    ]
    for store in stores:
        store.start()
    sums = jnp.sum(jnp.sum(heard_ref[...], axis=0), axis=1, keepdims=True)
    scale = rate * (jnp.sqrt(sums[0:1]) / jnp.sqrt(sums[1:2] + 1e-06))
    scale = jnp.broadcast_to(scale, (8, block))
    for k in range(rows_here // chunk):
        for r in range(k * chunk, (k + 1) * chunk, 8):
            for c in range(0, width, block):
                here = (pl.ds(r, 8), pl.ds(c, block))
                held_ref[here] = weights_ref[here] - scale * update_ref[here]
        rows = pl.ds(k * chunk, chunk)
        stores.append(pltpu.make_async_copy(held_ref.at[rows, :], out_ref.at[rows, :], sem.at[2 + k]))
        stores[-1].start()
    for store in stores:
        store.wait()


def local(weights, moment, second, tile_rows, row_index, bucket_count):
    owners = lax.axis_size(AXES)
    rows_here, width = weights.shape
    slot_total = row_index.shape[0]
    capacity = slot_total // owners
    block = math.gcd(width, 512)
    tile = math.gcd(width, 256)
    chunk = math.gcd(rows_here, 48)
    assert rows_here % 8 == 0 and rows_here <= 1 << 15
    table = jax.ShapeDtypeStruct((rows_here, width), jnp.float32)
    token = pl.pallas_call(
        start,
        out_shape=jax.ShapeDtypeStruct((8, LANES), jnp.float32),
        out_specs=VMEM,
        compiler_params=pltpu.CompilerParams(vmem_limit_bytes=MIB),
        cost_estimate=cost(10000000000),
        name="start",
    )()
    digits = pl.pallas_call(
        address,
        out_shape=jax.ShapeDtypeStruct((owners, capacity, LANES), jnp.bfloat16),
        in_specs=[VMEM] * 3,
        out_specs=VMEM,
        compiler_params=pltpu.CompilerParams(vmem_limit_bytes=4 * MIB),
        cost_estimate=cost(1000000),
        name="address",
    )(token, row_index, bucket_count)
    packed = pl.pallas_call(
        pack,
        out_shape=jax.ShapeDtypeStruct((owners, capacity, width + LANES), jnp.bfloat16),
        in_specs=[VMEM] * 2,
        out_specs=VMEM,
        compiler_params=pltpu.CompilerParams(vmem_limit_bytes=16 * MIB),
        cost_estimate=cost(10000000000),
        name="pack",
    )(digits, tile_rows)
    arrived = lax.all_to_all(packed, AXES, split_axis=0, concat_axis=0, tiled=True)
    late = jax.ShapeDtypeStruct((rows_here, block), jnp.float32)
    new_moment, new_second, late_moment, late_second, update, told = pl.pallas_call(
        functools.partial(advance, block, tile),
        out_shape=(table, table, late, late, table, jax.ShapeDtypeStruct((owners, 2, LANES), jnp.float32)),
        in_specs=[VMEM] * 4,
        out_specs=(ANY, ANY) + (VMEM,) * 4,
        scratch_shapes=[
            pltpu.VMEM((rows_here, width), jnp.float32),
            pltpu.VMEM((rows_here, width), jnp.float32),
            pltpu.VMEM((rows_here, block), jnp.float32),
            pltpu.VMEM((rows_here, block), jnp.float32),
            pltpu.SemaphoreType.DMA((2, width // block)),
        ],
        compiler_params=pltpu.CompilerParams(vmem_limit_bytes=32 * MIB),
        cost_estimate=cost(100000000),
        name="advance",
    )(arrived, weights, moment, second)
    heard = lax.all_to_all(told, AXES, split_axis=0, concat_axis=0, tiled=True)
    return pl.pallas_call(
        functools.partial(apply, chunk),
        out_shape=(table,) * 3,
        in_specs=[VMEM] * 5 + [ANY] * 2,
        out_specs=(ANY,) * 3,
        input_output_aliases={5: 1, 6: 2},
        scratch_shapes=[
            pltpu.VMEM((rows_here, width), jnp.float32),
            pltpu.SemaphoreType.DMA((2 + rows_here // chunk,)),
        ],
        compiler_params=pltpu.CompilerParams(vmem_limit_bytes=24 * MIB),
        cost_estimate=cost(1000000),
        name="apply",
    )(heard, weights, update, late_moment, late_second, new_moment, new_second)


def solution(mesh):
    placed = (P(AXES, None),) * 4 + (P(AXES),) * 2
    return jax.shard_map(
        local, mesh=mesh, in_specs=placed, out_specs=(P(AXES, None),) * 3, check_vma=False
    )
```

```python
import functools
import itertools
import math

import jax
import jax.numpy as jnp
from jax import lax
from jax.experimental import pallas as pl
from jax.experimental.pallas import tpu as pltpu
from jax.sharding import PartitionSpec as P

beta_one = 0.9
beta_two = 0.999
epsilon = 1e-06
decay = 0.01
rate = 0.1
LANES = 128
AXES = ("rows", "dp")
MIB = 1 << 20

VMEM = pl.BlockSpec(memory_space=pltpu.VMEM)
ANY = pl.BlockSpec(memory_space=pl.ANY)


def cost(flops):
    return pl.CostEstimate(flops=flops, bytes_accessed=0, transcendentals=0)


def start(token_ref):
    token_ref[...] = jnp.zeros_like(token_ref)


def address(token_ref, index_ref, count_ref, out_ref):
    del token_ref
    owners, capacity, lanes = out_ref.shape
    slots = owners * capacity
    slot = lax.broadcasted_iota(jnp.int32, (slots, slots), 0)
    across = lax.broadcasted_iota(jnp.int32, (slots, slots), 1)
    index = jnp.broadcast_to(index_ref[...].reshape(1, slots), (slots, slots))
    index = jnp.sum(jnp.where(slot == across, index, 0), axis=1, keepdims=True)
    owner = lax.broadcasted_iota(jnp.int32, (slots, owners), 0) // capacity
    across = lax.broadcasted_iota(jnp.int32, (slots, owners), 1)
    count = jnp.broadcast_to(count_ref[...].reshape(1, owners), (slots, owners))
    count = jnp.sum(jnp.where(owner == across, count, 0), axis=1, keepdims=True)
    place = lax.broadcasted_iota(jnp.int32, (slots, 1), 0) % capacity
    target = jnp.broadcast_to(jnp.where(place < count, index, -1), (slots, lanes))
    lane = lax.broadcasted_iota(jnp.int32, (slots, lanes), 1)
    digits = jnp.where(lane == 0, target >> 7, target & 127)
    digits = digits.astype(jnp.float32).astype(jnp.bfloat16)
    out_ref[...] = digits.reshape(owners, capacity, lanes)


def pack(digits_ref, tile_ref, out_ref):
    owners, capacity, padded = out_ref.shape
    width = padded - LANES
    out_ref[:, :, width:] = digits_ref[...]
    out_ref[:, :, :width] = tile_ref[...].reshape(owners, capacity, width)


def advance(block, tile, arrived_ref, weights_ref, moment_ref, second_ref,
            new_moment_hbm, new_second_hbm, late_moment_ref, late_second_ref, update_ref, told_ref,
            new_moment_ref, new_second_ref, even_ref, odd_ref, sem):
    rows_here, width = weights_ref.shape
    owners, capacity, _ = arrived_ref.shape
    slots = owners * capacity
    blocks = width // block
    digits = arrived_ref[:, :, width:].reshape(slots, LANES).astype(jnp.float32)
    landing = (digits[:, 0:1] * 128.0 + digits[:, 1:2]).astype(jnp.int32)
    picker = (
        landing == lax.broadcasted_iota(jnp.int32, (slots, rows_here), 1)
    ).astype(jnp.float32).T.astype(jnp.bfloat16)

    def gather(j, gradient_ref):
        for k in range(0, block, tile):
            sent = arrived_ref[:, :, j * block + k:j * block + k + tile].reshape(slots, tile)
            gradient_ref[:, k:k + tile] = jnp.dot(picker, sent, preferred_element_type=jnp.float32)

    weight_sum = jnp.zeros((8, tile), jnp.float32)
    update_sum = jnp.zeros((8, tile), jnp.float32)
    stores = []
    gather(0, even_ref)
    for j in range(blocks):
        gradient_ref, next_ref = (even_ref, odd_ref) if j % 2 == 0 else (odd_ref, even_ref)
        if j + 1 < blocks:
            gather(j + 1, next_ref)
        cols = pl.ds(j * block, block)
        late = j + 1 == blocks
        moment_to, second_to = (late_moment_ref, late_second_ref) if late else (new_moment_ref, new_second_ref)
        for r, c in itertools.product(range(0, rows_here, 8), range(0, block, tile)):
            rows, some = pl.ds(r, 8), pl.ds(j * block + c, tile)
            into = pl.ds(c, tile) if late else some
            gradient = gradient_ref[rows, pl.ds(c, tile)]
            weights = weights_ref[rows, some]
            new_moment = beta_one * moment_ref[rows, some] + (1.0 - beta_one) * gradient
            new_second = beta_two * second_ref[rows, some] + (1.0 - beta_two) * gradient * gradient
            root = new_second * lax.rsqrt(new_second)
            update = new_moment / (root + epsilon) + decay * weights
            moment_to[rows, into] = new_moment
            second_to[rows, into] = new_second
            update_ref[rows, some] = update
            weight_sum += weights * weights
            update_sum += update * update
        if late:
            continue
        for k, (held, out) in enumerate(((new_moment_ref, new_moment_hbm), (new_second_ref, new_second_hbm))):
            stores.append(pltpu.make_async_copy(held.at[:, cols], out.at[:, cols], sem.at[k, j]))
            stores[-1].start()

    def narrow(x):
        x = jnp.sum(x, axis=0, keepdims=True)
        return sum(x[:, k:k + LANES] for k in range(0, tile, LANES))

    both = jnp.concatenate([narrow(weight_sum), narrow(update_sum)], axis=0)
    told_ref[...] = jnp.broadcast_to(both[None], told_ref.shape)
    for store in stores:
        store.wait()


def apply(chunk, heard_ref, weights_ref, update_ref, late_moment_ref, late_second_ref, moment_in, second_in,
          out_ref, new_moment_hbm, new_second_hbm, held_ref, sem):
    del moment_in, second_in
    rows_here, width = weights_ref.shape
    block = late_moment_ref.shape[1]
    cols = pl.ds(width - block, block)
    stores = [
        pltpu.make_async_copy(late_moment_ref, new_moment_hbm.at[:, cols], sem.at[0]),
        pltpu.make_async_copy(late_second_ref, new_second_hbm.at[:, cols], sem.at[1]),
    ]
    for store in stores:
        store.start()
    sums = jnp.sum(jnp.sum(heard_ref[...], axis=0), axis=1, keepdims=True)
    scale = rate * (jnp.sqrt(sums[0:1]) / jnp.sqrt(sums[1:2] + 1e-06))
    scale = jnp.broadcast_to(scale, (8, block))
    for k in range(rows_here // chunk):
        for r in range(k * chunk, (k + 1) * chunk, 8):
            for c in range(0, width, block):
                here = (pl.ds(r, 8), pl.ds(c, block))
                held_ref[here] = weights_ref[here] - scale * update_ref[here]
        rows = pl.ds(k * chunk, chunk)
        stores.append(pltpu.make_async_copy(held_ref.at[rows, :], out_ref.at[rows, :], sem.at[2 + k]))
        stores[-1].start()
    for store in stores:
        store.wait()


def local(weights, moment, second, tile_rows, row_index, bucket_count):
    owners = lax.axis_size(AXES)
    rows_here, width = weights.shape
    slot_total = row_index.shape[0]
    capacity = slot_total // owners
    block = math.gcd(width, 512)
    tile = math.gcd(width, 256)
    chunk = math.gcd(rows_here, 48)
    assert rows_here % 8 == 0 and rows_here <= 1 << 15
    table = jax.ShapeDtypeStruct((rows_here, width), jnp.float32)
    token = pl.pallas_call(
        start,
        out_shape=jax.ShapeDtypeStruct((8, LANES), jnp.float32),
        out_specs=VMEM,
        compiler_params=pltpu.CompilerParams(vmem_limit_bytes=MIB),
        cost_estimate=cost(10000000000),
        name="start",
    )()
    digits = pl.pallas_call(
        address,
        out_shape=jax.ShapeDtypeStruct((owners, capacity, LANES), jnp.bfloat16),
        in_specs=[VMEM] * 3,
        out_specs=VMEM,
        compiler_params=pltpu.CompilerParams(vmem_limit_bytes=4 * MIB),
        cost_estimate=cost(1000000),
        name="address",
    )(token, row_index, bucket_count)
    packed = pl.pallas_call(
        pack,
        out_shape=jax.ShapeDtypeStruct((owners, capacity, width + LANES), jnp.bfloat16),
        in_specs=[VMEM] * 2,
        out_specs=VMEM,
        compiler_params=pltpu.CompilerParams(vmem_limit_bytes=16 * MIB),
        cost_estimate=cost(10000000000),
        name="pack",
    )(digits, tile_rows)
    arrived = lax.all_to_all(packed, AXES, split_axis=0, concat_axis=0, tiled=True)
    late = jax.ShapeDtypeStruct((rows_here, block), jnp.float32)
    new_moment, new_second, late_moment, late_second, update, told = pl.pallas_call(
        functools.partial(advance, block, tile),
        out_shape=(table, table, late, late, table, jax.ShapeDtypeStruct((owners, 2, LANES), jnp.float32)),
        in_specs=[VMEM] * 4,
        out_specs=(ANY, ANY) + (VMEM,) * 4,
        scratch_shapes=[
            pltpu.VMEM((rows_here, width), jnp.float32),
            pltpu.VMEM((rows_here, width), jnp.float32),
            pltpu.VMEM((rows_here, block), jnp.float32),
            pltpu.VMEM((rows_here, block), jnp.float32),
            pltpu.SemaphoreType.DMA((2, width // block)),
        ],
        compiler_params=pltpu.CompilerParams(vmem_limit_bytes=32 * MIB),
        cost_estimate=cost(100000000),
        name="advance",
    )(arrived, weights, moment, second)
    heard = lax.all_to_all(told, AXES, split_axis=0, concat_axis=0, tiled=True)
    return pl.pallas_call(
        functools.partial(apply, chunk),
        out_shape=(table,) * 3,
        in_specs=[VMEM] * 5 + [ANY] * 2,
        out_specs=(ANY,) * 3,
        input_output_aliases={5: 1, 6: 2},
        scratch_shapes=[
            pltpu.VMEM((rows_here, width), jnp.float32),
            pltpu.SemaphoreType.DMA((2 + rows_here // chunk,)),
        ],
        compiler_params=pltpu.CompilerParams(vmem_limit_bytes=24 * MIB),
        cost_estimate=cost(1000000),
        name="apply",
    )(heard, weights, update, late_moment, late_second, new_moment, new_second)


def solution(mesh):
    placed = (P(AXES, None),) * 4 + (P(AXES),) * 2
    return jax.shard_map(
        local, mesh=mesh, in_specs=placed, out_specs=(P(AXES, None),) * 3, check_vma=False
    )
```
